32 devices in a mesh: zero: 8 (over y, x, core), width: 4 (over z).
Axes of the slice: x: 2, y: 2, z: 4, core: 2. Of those that a mesh axis runs over, the one named last changes fastest.
Arguments:
- train_query: bfloat16 [4608, 4096], P('zero', 'width'), may hold values from -0.09375 to 0.09375
- low_query: bfloat16 [4608, 64], P('zero'), may hold values from -0.09375 to 0.09375
- high_query: bfloat16 [64, 4096], P(None, 'width'), may hold values from -0.75 to 0.75
- train_key: bfloat16 [4608, 2048], P('zero', 'width'), may hold values from -0.09375 to 0.09375
- low_key: bfloat16 [4608, 64], P('zero'), may hold values from -0.09375 to 0.09375
- high_key: bfloat16 [64, 2048], P(None, 'width'), may hold values from -0.75 to 0.75
- train_value: bfloat16 [4608, 2048], P('zero', 'width'), may hold values from -0.09375 to 0.09375
- low_value: bfloat16 [4608, 64], P('zero'), may hold values from -0.09375 to 0.09375
- high_value: bfloat16 [64, 2048], P(None, 'width'), may hold values from -0.75 to 0.75
- train_mixed: bfloat16 [4096, 4608], P('width', 'zero'), may hold values from -0.09375 to 0.09375
- low_mixed: bfloat16 [4096, 64], P('width'), may hold values from -0.09375 to 0.09375
- high_mixed: bfloat16 [64, 4608], P(None, 'zero'), may hold values from -0.75 to 0.75
- norm_train: float32 [4608], P(('zero', 'width')), may hold values from 0.25 to 1.75
- norm_step: float32 [4608], P(('zero', 'width')), may hold values from -0.3 to 0.3
Outputs:
- final_query: bfloat16 [4608, 4096], P(None, 'width')
- final_key: bfloat16 [4608, 2048], P(None, 'width')
- final_value: bfloat16 [4608, 2048], P(None, 'width')
- final_mixed: bfloat16 [4096, 4608], P('width')
- serve_norm: bfloat16 [4608], replicated
The draws below stay inside these ranges and needn't reach their ends.
All inputs are finite; a program needn't handle non-finite values.
Results may differ from the reference program's by a relative error of at most 0.001.
Values may be sent and summed in bfloat16 or wider, within the bound.
A program may use at most 192 MiB of HBM per device.

```python
import jax
import jax.numpy as jnp

D_MODEL = 4608
Q_DIM = 4096
KV_DIM = 2048
RANK = 64


def levels(stream_key, dims, pieces, low, largest):
    def one(position, parts):
        draws = jax.random.uniform(jax.random.fold_in(jax.random.fold_in(stream_key, 6), position), (parts,), jnp.float32, low / len(pieces), largest / len(pieces))
        return jnp.repeat(jnp.exp(draws), dims[position] // parts).reshape((-1,) + (1,) * (len(dims) - position - 1))

    loudness = one(*pieces[0])
    for cut in pieces[1:]:
        loudness = loudness * one(*cut)
    return loudness


def gaussian(key, shape, scale, bound, pieces=(), held_as=jnp.bfloat16):
    result = jax.random.normal(key, shape, jnp.float32) * scale
    if len(pieces) > 0:
        result = levels(key, shape, pieces, -0.22, 0.18) * result
    return jnp.clip(result, min=-bound, max=bound).astype(held_as)


def setup_inputs(seed: int = 0) -> dict:
    key_of = jax.random.split(jax.random.key(seed), 15)
    train_query = gaussian(key_of[0], (D_MODEL, Q_DIM), D_MODEL ** -0.5, 0.09375, ((0, 8), (1, 4)))
    low_query = gaussian(key_of[1], (D_MODEL, RANK), D_MODEL ** -0.5, 0.09375, ((0, 8),))
    high_query = gaussian(key_of[2], (RANK, Q_DIM), RANK ** -0.5, 0.75, ((1, 4),))
    train_key = gaussian(key_of[3], (D_MODEL, KV_DIM), D_MODEL ** -0.5, 0.09375, ((0, 8), (1, 4)))
    low_key = gaussian(key_of[4], (D_MODEL, RANK), D_MODEL ** -0.5, 0.09375, ((0, 8),))
    high_key = gaussian(key_of[5], (RANK, KV_DIM), RANK ** -0.5, 0.75, ((1, 4),))
    train_value = gaussian(key_of[6], (D_MODEL, KV_DIM), D_MODEL ** -0.5, 0.09375, ((0, 8), (1, 4)))
    low_value = gaussian(key_of[7], (D_MODEL, RANK), D_MODEL ** -0.5, 0.09375, ((0, 8),))
    high_value = gaussian(key_of[8], (RANK, KV_DIM), RANK ** -0.5, 0.75, ((1, 4),))
    train_mixed = gaussian(key_of[9], (Q_DIM, D_MODEL), Q_DIM ** -0.5, 0.09375, ((0, 4), (1, 8)))
    low_mixed = gaussian(key_of[10], (Q_DIM, RANK), Q_DIM ** -0.5, 0.09375, ((0, 4),))
    high_mixed = gaussian(key_of[11], (RANK, D_MODEL), RANK ** -0.5, 0.75, ((1, 8),))
    norm_train = jnp.clip(1.0 + 0.15 * jax.random.normal(key_of[12], (D_MODEL,), jnp.float32), 0.25, 1.75)
    norm_step = jnp.clip(jax.random.uniform(key_of[13], (D_MODEL,), jnp.float32, -0.3, 0.3) * levels(key_of[13], (D_MODEL,), ((0, 32),), -0.4, 0.0), -0.3, 0.3)
    return {"train_query": train_query, "low_query": low_query, "high_query": high_query, "train_key": train_key, "low_key": low_key, "high_key": high_key, "train_value": train_value, "low_value": low_value, "high_value": high_value, "train_mixed": train_mixed, "low_mixed": low_mixed, "high_mixed": high_mixed, "norm_train": norm_train, "norm_step": norm_step}


mix_rate = 0.5


def reference(train_query, low_query, high_query, train_key, low_key, high_key, train_value, low_value, high_value, train_mixed, low_mixed, high_mixed, norm_train, norm_step):
    result_query = train_query.astype(jnp.float32) + mix_rate * jnp.dot(low_query, high_query, preferred_element_type=jnp.float32)
    result_key = train_key.astype(jnp.float32) + mix_rate * jnp.dot(low_key, high_key, preferred_element_type=jnp.float32)
    result_value = train_value.astype(jnp.float32) + mix_rate * jnp.dot(low_value, high_value, preferred_element_type=jnp.float32)
    result_mixed = train_mixed.astype(jnp.float32) + mix_rate * jnp.dot(low_mixed, high_mixed, preferred_element_type=jnp.float32)
    final_query = result_query.astype(jnp.bfloat16)
    final_key = result_key.astype(jnp.bfloat16)
    final_value = result_value.astype(jnp.bfloat16)
    final_mixed = result_mixed.astype(jnp.bfloat16)
    serve_norm = (norm_train + norm_step).astype(jnp.bfloat16)
    return final_query, final_key, final_value, final_mixed, serve_norm
```

```python
import functools
import math

import jax
import jax.numpy as jnp
from jax import lax
from jax.experimental import pallas as pl
from jax.experimental.pallas import tpu as pltpu
from jax.sharding import PartitionSpec as P

mix_rate = 0.5
MESH = pl.DeviceIdType.MESH


def gather_kernel(n, width, *refs):
    trains, lows, highs, norm = refs[0:4], refs[4:8], refs[8:12], refs[12]
    outs, norm_out = refs[13:17], refs[17]
    mine, norm_row = refs[18:22], refs[22]
    send_sem, recv_sem, norm_send, norm_recv, local_sem = refs[23:28]

    chips = n // 2
    side = math.isqrt(chips)
    if side * side != chips:
        side = chips
    rows = trains[0].shape[0]
    half = rows // 2

    me = lax.axis_index("zero")
    me_width = lax.axis_index("width")
    chip, core = me // 2, me % 2

    def turned(place):
        y, x = place // side, place % side
        return y * side + x + (y % 2) * (side - 1 - 2 * x)

    ring = turned(chip)

    def at(step):
        return turned((ring + step + chips) % chips) * 2 + core

    after, before = at(1), at(-1)
    partner = chip * 2 + (1 - core)

    barrier = pltpu.get_barrier_semaphore()
    for step in range(1, n):
        pl.semaphore_signal(
            barrier, inc=1, device_id={"zero": (me + step) % n}, device_id_type=MESH
        )
    for step in range(1, width):
        pl.semaphore_signal(
            barrier, inc=1, device_id={"width": (me_width + step) % width}, device_id_type=MESH
        )

    started = []
    locals_ = []
    count = [0]

    def block(array, owner, part):
        return outs[array].at[pl.ds(pl.multiple_of(owner * rows + part * half, 8), half)]

    def send(source, target, device):
        slot = count[0]
        count[0] += 1
        copy = pltpu.make_async_remote_copy(
            src_ref=source,
            dst_ref=target,
            send_sem=send_sem.at[slot],
            recv_sem=recv_sem.at[slot],
            device_id={"zero": device},
            device_id_type=MESH,
        )
        copy.start()
        started.append(copy)
        return copy

    def own(array, part):
        return mine[array].at[pl.ds(part * half, half)]

    def compute(array):
        delta = lax.dot_general(
            lows[array][...],
            highs[array][...],
            (((0,), (0,)), ((), ())),
            preferred_element_type=jnp.float32,
        )
        merged = trains[array][...].astype(jnp.float32) + mix_rate * delta
        mine[array][...] = merged.astype(jnp.bfloat16)

    streams = ([], [])
    aways = (after, before)
    partner_copies = []
    hops = chips // 2

    def send_own(direction, array, part):
        copy = send(own(array, part), block(array, me, part), aways[direction])
        streams[direction].append((copy, array, part))

    for array in range(4):
        compute(array)
        if array == 0:
            pl.semaphore_wait(barrier, n - 1 + width - 1)
        send_own(0, array, 0)
        send_own(1, array, 1)
    if hops > 1:
        for array in range(4):
            send_own(0, array, 1)
            send_own(1, array, 0)

    own_row = pltpu.make_async_copy(norm, norm_row.at[me_width], local_sem.at[4])
    own_row.start()
    row_copies = []
    for step in range(1, width):
        copy = pltpu.make_async_remote_copy(
            src_ref=norm,
            dst_ref=norm_row.at[me_width],
            send_sem=norm_send.at[step - 1],
            recv_sem=norm_recv.at[step - 1],
            device_id={"width": (me_width + step) % width},
            device_id_type=MESH,
        )
        copy.start()
        row_copies.append(copy)

    for array in range(4):
        copy = pltpu.make_async_copy(
            mine[array],
            outs[array].at[pl.ds(pl.multiple_of(me * rows, 8), rows)],
            local_sem.at[array],
        )
        copy.start()
        locals_.append(copy)
        for part in range(2):
            partner_copies.append(send(own(array, part), block(array, me, part), partner))

    own_row.wait()
    for copy in row_copies:
        copy.wait()
    own_table = pltpu.make_async_copy(norm_row, norm_out.at[me], local_sem.at[4])
    own_table.start()
    table_copies = []
    for step in range(1, n):
        copy = pltpu.make_async_remote_copy(
            src_ref=norm_row,
            dst_ref=norm_out.at[me],
            send_sem=norm_send.at[width - 2 + step],
            recv_sem=norm_recv.at[width - 2 + step],
            device_id={"zero": (me + step) % n},
            device_id_type=MESH,
        )
        copy.start()
        table_copies.append(copy)

    for hop in range(1, hops + 1):
        arriving = streams
        streams = ([], [])
        for turn in range(len(arriving[0])):
            for direction in range(2):
                copy, array, part = arriving[direction][turn]
                owner = at(-hop if direction == 0 else hop)
                copy.wait_recv()
                here = block(array, owner, part)
                last = hop + 1 == hops
                if hop < hops and (not last or part == direction):
                    further = send(here, here, aways[direction])
                    streams[direction].append((further, array, part))
                partner_copies.append(send(here, here, partner))

    for copy in partner_copies:
        copy.wait_recv()
    for copy in started:
        copy.wait_send()
    for copy in table_copies:
        copy.wait()
    own_table.wait()
    for copy in locals_:
        copy.wait()


def gather(n, width, trains, lows, highs, norm):
    chips = n // 2
    hops = chips // 2
    ring_blocks = 2 * (8 * (hops - 1) + 4)
    slots = ring_blocks + 8 + ring_blocks
    vmem = pl.BlockSpec(memory_space=pltpu.VMEM)
    anywhere = pl.BlockSpec(memory_space=pl.ANY)
    return pl.pallas_call(
        functools.partial(gather_kernel, n, width),
        out_shape=[
            jax.ShapeDtypeStruct((n * train.shape[0], train.shape[1]), jnp.bfloat16)
            for train in trains
        ]
        + [jax.ShapeDtypeStruct((n, width) + norm.shape, norm.dtype)],
        in_specs=[vmem] * 13,
        out_specs=[anywhere] * 5,
        scratch_shapes=[pltpu.VMEM(train.shape, jnp.bfloat16) for train in trains]
        + [
            pltpu.VMEM((width,) + norm.shape, norm.dtype),
            pltpu.SemaphoreType.DMA((slots,)),
            pltpu.SemaphoreType.DMA((slots,)),
            pltpu.SemaphoreType.DMA((n + width - 2,)),
            pltpu.SemaphoreType.DMA((n + width - 2,)),
            pltpu.SemaphoreType.DMA((5,)),
        ],
        compiler_params=pltpu.CompilerParams(collective_id=0, has_side_effects=True),
    )(*trains, *lows, *highs, norm)


def on_device(
    n,
    width,
    train_query,
    low_query,
    high_query,
    train_key,
    low_key,
    high_key,
    train_value,
    low_value,
    high_value,
    train_mixed,
    low_mixed,
    high_mixed,
    norm_train,
    norm_step,
):
    share = norm_train.shape[0]
    lanes = -(-share // 1024) * 1024
    norm = jnp.pad(norm_train + norm_step, (0, lanes - share)).reshape(-1, 128)
    query, key, value, mixed, table = gather(
        n,
        width,
        (train_query, train_key, train_value, train_mixed.T),
        (low_query.T, low_key.T, low_value.T, high_mixed),
        (high_query, high_key, high_value, low_mixed.T),
        norm,
    )
    serve_norm = table.reshape(n * width, -1)[:, :share].reshape(-1).astype(jnp.bfloat16)
    return (query, key, value, mixed.T, serve_norm)


def solution(mesh):
    return jax.shard_map(
        functools.partial(on_device, mesh.shape["zero"], mesh.shape["width"]),
        mesh=mesh,
        in_specs=(
            P("zero", "width"),
            P("zero", None),
            P(None, "width"),
            P("zero", "width"),
            P("zero", None),
            P(None, "width"),
            P("zero", "width"),
            P("zero", None),
            P(None, "width"),
            P("width", "zero"),
            P("width", None),
            P(None, "zero"),
            P(("zero", "width")),
            P(("zero", "width")),
        ),
        out_specs=(P(None, "width"), P(None, "width"), P(None, "width"), P("width", None), P()),
        check_vma=False,
    )
```

```python
import functools
import math

import jax
import jax.numpy as jnp
from jax import lax
from jax.experimental import pallas as pl
from jax.experimental.pallas import tpu as pltpu
from jax.sharding import PartitionSpec as P

mix_rate = 0.5
PIECES = 4
GATHER_VMEM = 30 * 1024 * 1024
MESH = pl.DeviceIdType.MESH


def gather_kernel(n, width, *refs):
    trains, lows, highs, norm = refs[0:4], refs[4:8], refs[8:12], refs[12]
    turned_mixed, norm_out = refs[13], refs[17]
    mine, mixed, norm_row = refs[18:22], refs[22], refs[23]
    outs = (mixed,) + tuple(refs[14:17])
    send_sem, recv_sem, norm_send, norm_recv, local_sem = refs[24:29]

    chips = n // 2
    side = math.isqrt(chips)
    if side * side != chips:
        side = chips
    rows = trains[0].shape[0]
    half = rows // 2

    me = lax.axis_index("zero")
    me_width = lax.axis_index("width")
    chip, core = me // 2, me % 2

    def turned(place):
        y, x = place // side, place % side
        return y * side + x + (y % 2) * (side - 1 - 2 * x)

    ring = turned(chip)

    def at(step):
        return turned((ring + step + chips) % chips) * 2 + core

    after, before = at(1), at(-1)
    partner = chip * 2 + (1 - core)

    barrier = pltpu.get_barrier_semaphore()
    for step in range(1, n):
        pl.semaphore_signal(
            barrier, inc=1, device_id={"zero": (me + step) % n}, device_id_type=MESH
        )
    for step in range(1, width):
        pl.semaphore_signal(
            barrier, inc=1, device_id={"width": (me_width + step) % width}, device_id_type=MESH
        )

    started = []
    locals_ = []
    count = [0]

    def block(array, owner, part):
        return outs[array].at[pl.ds(pl.multiple_of(owner * rows + part * half, 8), half)]

    def send(source, target, device):
        slot = count[0]
        count[0] += 1
        copy = pltpu.make_async_remote_copy(
            src_ref=source,
            dst_ref=target,
            send_sem=send_sem.at[slot],
            recv_sem=recv_sem.at[slot],
            device_id={"zero": device},
            device_id_type=MESH,
        )
        copy.start()
        started.append(copy)
        return copy

    def own(array, part):
        return mine[array].at[pl.ds(part * half, half)]

    def compute(array):
        delta = lax.dot_general(
            lows[array][...],
            highs[array][...],
            (((0,), (0,)), ((), ())),
            preferred_element_type=jnp.float32,
        )
        merged = trains[array][...].astype(jnp.float32) + mix_rate * delta
        mine[array][...] = merged.astype(jnp.bfloat16)

    streams = ([], [])
    aways = (after, before)
    partner_copies = []
    mixed_copies = {}
    pair = 2 * rows
    per_chip = pair % 128 == 0

    def forward(source, target, array, step):
        copy = send(source, target, partner)
        if array == 0 and per_chip:
            mixed_copies.setdefault(step % chips, []).append(copy)
        else:
            partner_copies.append(copy)

    def turn_columns(start, tiles):
        def one(tile, carry):
            place = pl.ds(pl.multiple_of(start + tile * 128, 128), 128)
            turned_mixed[:, place] = mixed[place, :].T
            return carry

        lax.fori_loop(0, tiles, one, 0)

    def turn_chip(step):
        if per_chip:
            for copy in mixed_copies.pop(step % chips):
                copy.wait_recv()
            if step == 0:
                locals_[0].wait()
            turn_columns((at(step) // 2) * pair, pair // 128)

    hops = chips // 2

    def send_own(direction, array, part):
        copy = send(own(array, part), block(array, me, part), aways[direction])
        streams[direction].append((copy, array, part))

    for array in range(4):
        compute(array)
        if array == 0:
            pl.semaphore_wait(barrier, n - 1 + width - 1)
        send_own(0, array, 0)
        send_own(1, array, 1)
    if hops > 1:
        for array in range(4):
            send_own(0, array, 1)
            send_own(1, array, 0)

    own_row = pltpu.make_async_copy(norm, norm_row.at[me_width], local_sem.at[4])
    own_row.start()
    row_copies = []
    for step in range(1, width):
        copy = pltpu.make_async_remote_copy(
            src_ref=norm,
            dst_ref=norm_row.at[me_width],
            send_sem=norm_send.at[step - 1],
            recv_sem=norm_recv.at[step - 1],
            device_id={"width": (me_width + step) % width},
            device_id_type=MESH,
        )
        copy.start()
        row_copies.append(copy)

    for array in range(4):
        copy = pltpu.make_async_copy(
            mine[array],
            outs[array].at[pl.ds(pl.multiple_of(me * rows, 8), rows)],
            local_sem.at[array],
        )
        copy.start()
        locals_.append(copy)
        for part in range(2):
            forward(own(array, part), block(array, me, part), array, 0)

    own_row.wait()
    for copy in row_copies:
        copy.wait()
    own_table = pltpu.make_async_copy(norm_row, norm_out.at[me], local_sem.at[4])
    own_table.start()
    table_copies = []
    for step in range(1, n):
        copy = pltpu.make_async_remote_copy(
            src_ref=norm_row,
            dst_ref=norm_out.at[me],
            send_sem=norm_send.at[width - 2 + step],
            recv_sem=norm_recv.at[width - 2 + step],
            device_id={"zero": (me + step) % n},
            device_id_type=MESH,
        )
        copy.start()
        table_copies.append(copy)

    turn_chip(0)

    for hop in range(1, hops + 1):
        arriving = streams
        streams = ([], [])
        for turn in range(len(arriving[0])):
            for direction in range(2):
                copy, array, part = arriving[direction][turn]
                owner = at(-hop if direction == 0 else hop)
                copy.wait_recv()
                here = block(array, owner, part)
                last = hop + 1 == hops
                if hop < hops and (not last or part == direction):
                    further = send(here, here, aways[direction])
                    streams[direction].append((further, array, part))
                forward(here, here, array, hop if direction else -hop)
            if hop == hops and turn == 1:
                turn_chip(hop)
        if hop < hops:
            turn_chip(-hop)
            turn_chip(hop)

    for copy in partner_copies:
        copy.wait_recv()
    for copy in started:
        copy.wait_send()
    for copy in table_copies:
        copy.wait()
    own_table.wait()
    for copy in locals_[1 if per_chip else 0 :]:
        copy.wait()
    if not per_chip:
        turn_columns(0, n * rows // 128)


def gather(n, width, trains, lows, highs, norm):
    chips = n // 2
    hops = chips // 2
    ring_blocks = 2 * (8 * (hops - 1) + 4)
    slots = ring_blocks + 8 + ring_blocks
    vmem = pl.BlockSpec(memory_space=pltpu.VMEM)
    anywhere = pl.BlockSpec(memory_space=pl.ANY)
    return pl.pallas_call(
        functools.partial(gather_kernel, n, width),
        out_shape=[pltpu.VMEM(trains[0].shape[1:] + (n * trains[0].shape[0],), jnp.bfloat16)]
        + [
            pltpu.VMEM((n * train.shape[0], train.shape[1]), jnp.bfloat16) for train in trains[1:]
        ]
        + [jax.ShapeDtypeStruct((n, width) + norm.shape, norm.dtype)],
        in_specs=[vmem] * 13,
        out_specs=[vmem] * 4 + [anywhere],
        scratch_shapes=[pltpu.VMEM(train.shape, jnp.bfloat16) for train in trains]
        + [
            pltpu.VMEM((n * trains[0].shape[0], trains[0].shape[1]), jnp.bfloat16),
            pltpu.VMEM((width,) + norm.shape, norm.dtype),
            pltpu.SemaphoreType.DMA((slots,)),
            pltpu.SemaphoreType.DMA((slots,)),
            pltpu.SemaphoreType.DMA((n + width - 2,)),
            pltpu.SemaphoreType.DMA((n + width - 2,)),
            pltpu.SemaphoreType.DMA((5,)),
        ],
        compiler_params=pltpu.CompilerParams(
            collective_id=0, has_side_effects=True, vmem_limit_bytes=GATHER_VMEM
        ),
    )(*trains, *lows, *highs, norm)


def write_kernel(*refs):
    arrays, sem = len(refs) // 2, refs[-1]
    copies = []
    for array in range(arrays):
        source, target = refs[array], refs[arrays + array]
        piece = source.shape[0] // PIECES
        for cut in range(PIECES):
            copy = pltpu.make_async_copy(
                source.at[pl.ds(cut * piece, piece)],
                target.at[pl.ds(cut * piece, piece)],
                sem.at[array * PIECES + cut],
            )
            copy.start()
            copies.append(copy)
    for copy in copies:
        copy.wait()


def write_out(arrays):
    return pl.pallas_call(
        write_kernel,
        out_shape=[jax.ShapeDtypeStruct(array.shape, array.dtype) for array in arrays],
        in_specs=[pl.BlockSpec(memory_space=pltpu.VMEM)] * len(arrays),
        out_specs=[pl.BlockSpec(memory_space=pltpu.HBM)] * len(arrays),
        scratch_shapes=[pltpu.SemaphoreType.DMA((len(arrays) * PIECES,))],
        compiler_params=pltpu.CompilerParams(vmem_limit_bytes=1024 * 1024),
    )(*arrays)


def on_device(
    n,
    width,
    train_query,
    low_query,
    high_query,
    train_key,
    low_key,
    high_key,
    train_value,
    low_value,
    high_value,
    train_mixed,
    low_mixed,
    high_mixed,
    norm_train,
    norm_step,
):
    share = norm_train.shape[0]
    lanes = -(-share // 1024) * 1024
    norm = jnp.pad(norm_train + norm_step, (0, lanes - share)).reshape(-1, 128)
    *gathered, table = gather(
        n,
        width,
        (train_mixed.T, train_query, train_key, train_value),
        (high_mixed, low_query.T, low_key.T, low_value.T),
        (low_mixed.T, high_query, high_key, high_value),
        norm,
    )
    mixed, query, key, value = write_out(gathered)
    serve_norm = table.reshape(n * width, -1)[:, :share].reshape(-1).astype(jnp.bfloat16)
    return (query, key, value, mixed, serve_norm)


def solution(mesh):
    return jax.shard_map(
        functools.partial(on_device, mesh.shape["zero"], mesh.shape["width"]),
        mesh=mesh,
        in_specs=(
            P("zero", "width"),
            P("zero", None),
            P(None, "width"),
            P("zero", "width"),
            P("zero", None),
            P(None, "width"),
            P("zero", "width"),
            P("zero", None),
            P(None, "width"),
            P("width", "zero"),
            P("width", None),
            P(None, "zero"),
            P(("zero", "width")),
            P(("zero", "width")),
        ),
        out_specs=(P(None, "width"), P(None, "width"), P(None, "width"), P("width", None), P()),
        check_vma=False,
    )
```

```python
import functools
import math

import jax
import jax.numpy as jnp
from jax import lax
from jax.experimental import pallas as pl
from jax.experimental.pallas import tpu as pltpu
from jax.sharding import PartitionSpec as P

mix_rate = 0.5
PIECES = 4
GATHER_VMEM = 30 * 1024 * 1024
MESH = pl.DeviceIdType.MESH


def gather_kernel(n, width, *refs):
    trains, lows, highs, norm = refs[0:4], refs[4:8], refs[8:12], refs[12]
    turned_mixed, norm_out = refs[13], refs[17]
    mine, mixed, norm_row = refs[18:22], refs[22], refs[23]
    outs = (mixed,) + tuple(refs[14:17])
    send_sem, recv_sem, norm_send, norm_recv, local_sem = refs[24:29]

    chips = n // 2
    side = math.isqrt(chips)
    if side * side != chips:
        side = chips
    rows = trains[0].shape[0]
    half = rows // 2

    me = lax.axis_index("zero")
    me_width = lax.axis_index("width")
    chip, core = me // 2, me % 2

    def turned(place):
        y, x = place // side, place % side
        return y * side + x + (y % 2) * (side - 1 - 2 * x)

    ring = turned(chip)

    def at(step):
        return turned((ring + step + chips) % chips) * 2 + core

    after, before = at(1), at(-1)
    partner = chip * 2 + (1 - core)

    loads = []
    for array in range(4):
        copy = pltpu.make_async_copy(trains[array], mine[array], local_sem.at[array])
        copy.start()
        loads.append(copy)

    barrier = pltpu.get_barrier_semaphore()
    for step in range(1, n):
        pl.semaphore_signal(
            barrier, inc=1, device_id={"zero": (me + step) % n}, device_id_type=MESH
        )
    for step in range(1, width):
        pl.semaphore_signal(
            barrier, inc=1, device_id={"width": (me_width + step) % width}, device_id_type=MESH
        )

    started = []
    locals_ = []
    count = [0]

    def block(array, owner, part):
        return outs[array].at[pl.ds(pl.multiple_of(owner * rows + part * half, 8), half)]

    def send(source, target, device):
        slot = count[0]
        count[0] += 1
        copy = pltpu.make_async_remote_copy(
            src_ref=source,
            dst_ref=target,
            send_sem=send_sem.at[slot],
            recv_sem=recv_sem.at[slot],
            device_id={"zero": device},
            device_id_type=MESH,
        )
        copy.start()
        started.append(copy)
        return copy

    def own(array, part):
        return mine[array].at[pl.ds(part * half, half)]

    def compute(array):
        delta = lax.dot_general(
            lows[array][...],
            highs[array][...],
            (((0,), (0,)), ((), ())),
            preferred_element_type=jnp.float32,
        )
        loads[array].wait()
        merged = mine[array][...].astype(jnp.float32) + mix_rate * delta
        mine[array][...] = merged.astype(jnp.bfloat16)

    streams = ([], [])
    aways = (after, before)
    partner_copies = []
    mixed_copies = {}
    pair = 2 * rows
    per_chip = pair % 128 == 0

    def forward(source, target, array, step):
        copy = send(source, target, partner)
        if array == 0 and per_chip:
            mixed_copies.setdefault(step % chips, []).append(copy)
        else:
            partner_copies.append(copy)

    def turn_columns(start, tiles):
        def one(tile, carry):
            place = pl.ds(pl.multiple_of(start + tile * 128, 128), 128)
            turned_mixed[:, place] = mixed[place, :].T
            return carry

        lax.fori_loop(0, tiles, one, 0)

    def turn_chip(step):
        if per_chip:
            for copy in mixed_copies.pop(step % chips):
                copy.wait_recv()
            if step == 0:
                locals_[0].wait()
            turn_columns((at(step) // 2) * pair, pair // 128)

    hops = chips // 2

    def send_own(direction, array, part):
        copy = send(own(array, part), block(array, me, part), aways[direction])
        streams[direction].append((copy, array, part))

    for array in range(4):
        compute(array)
        if array == 0:
            pl.semaphore_wait(barrier, n - 1 + width - 1)
        send_own(0, array, 0)
        send_own(1, array, 1)
    if hops > 1:
        for array in range(4):
            send_own(0, array, 1)
            send_own(1, array, 0)

    own_row = pltpu.make_async_copy(norm, norm_row.at[me_width], local_sem.at[4])
    own_row.start()
    row_copies = []
    for step in range(1, width):
        copy = pltpu.make_async_remote_copy(
            src_ref=norm,
            dst_ref=norm_row.at[me_width],
            send_sem=norm_send.at[step - 1],
            recv_sem=norm_recv.at[step - 1],
            device_id={"width": (me_width + step) % width},
            device_id_type=MESH,
        )
        copy.start()
        row_copies.append(copy)

    for array in range(4):
        copy = pltpu.make_async_copy(
            mine[array],
            outs[array].at[pl.ds(pl.multiple_of(me * rows, 8), rows)],
            local_sem.at[array],
        )
        copy.start()
        locals_.append(copy)
        for part in range(2):
            forward(own(array, part), block(array, me, part), array, 0)

    own_row.wait()
    for copy in row_copies:
        copy.wait()
    own_table = pltpu.make_async_copy(norm_row, norm_out.at[me], local_sem.at[4])
    own_table.start()
    table_copies = []
    for step in range(1, n):
        copy = pltpu.make_async_remote_copy(
            src_ref=norm_row,
            dst_ref=norm_out.at[me],
            send_sem=norm_send.at[width - 2 + step],
            recv_sem=norm_recv.at[width - 2 + step],
            device_id={"zero": (me + step) % n},
            device_id_type=MESH,
        )
        copy.start()
        table_copies.append(copy)

    turn_chip(0)

    for hop in range(1, hops + 1):
        arriving = streams
        streams = ([], [])
        for turn in range(len(arriving[0])):
            for direction in range(2):
                copy, array, part = arriving[direction][turn]
                owner = at(-hop if direction == 0 else hop)
                copy.wait_recv()
                here = block(array, owner, part)
                last = hop + 1 == hops
                if hop < hops and (not last or part == direction):
                    further = send(here, here, aways[direction])
                    streams[direction].append((further, array, part))
                forward(here, here, array, hop if direction else -hop)
            if hop == hops and turn == 1:
                turn_chip(hop)
        if hop < hops:
            turn_chip(-hop)
            turn_chip(hop)

    for copy in partner_copies:
        copy.wait_recv()
    for copy in started:
        copy.wait_send()
    for copy in table_copies:
        copy.wait()
    own_table.wait()
    for copy in locals_[1 if per_chip else 0 :]:
        copy.wait()
    if not per_chip:
        turn_columns(0, n * rows // 128)


def gather(n, width, trains, lows, highs, norm):
    chips = n // 2
    hops = chips // 2
    ring_blocks = 2 * (8 * (hops - 1) + 4)
    slots = ring_blocks + 8 + ring_blocks
    vmem = pl.BlockSpec(memory_space=pltpu.VMEM)
    anywhere = pl.BlockSpec(memory_space=pl.ANY)
    return pl.pallas_call(
        functools.partial(gather_kernel, n, width),
        out_shape=[pltpu.VMEM(trains[0].shape[1:] + (n * trains[0].shape[0],), jnp.bfloat16)]
        + [
            pltpu.VMEM((n * train.shape[0], train.shape[1]), jnp.bfloat16) for train in trains[1:]
        ]
        + [jax.ShapeDtypeStruct((n, width) + norm.shape, norm.dtype)],
        in_specs=[anywhere] * 4 + [vmem] * 9,
        out_specs=[vmem] * 4 + [anywhere],
        scratch_shapes=[pltpu.VMEM(train.shape, jnp.bfloat16) for train in trains]
        + [
            pltpu.VMEM((n * trains[0].shape[0], trains[0].shape[1]), jnp.bfloat16),
            pltpu.VMEM((width,) + norm.shape, norm.dtype),
            pltpu.SemaphoreType.DMA((slots,)),
            pltpu.SemaphoreType.DMA((slots,)),
            pltpu.SemaphoreType.DMA((n + width - 2,)),
            pltpu.SemaphoreType.DMA((n + width - 2,)),
            pltpu.SemaphoreType.DMA((5,)),
        ],
        compiler_params=pltpu.CompilerParams(
            collective_id=0, has_side_effects=True, vmem_limit_bytes=GATHER_VMEM
        ),
    )(*trains, *lows, *highs, norm)


def write_kernel(*refs):
    arrays, sem = len(refs) // 2, refs[-1]
    copies = []
    for array in range(arrays):
        source, target = refs[array], refs[arrays + array]
        piece = source.shape[0] // PIECES
        for cut in range(PIECES):
            copy = pltpu.make_async_copy(
                source.at[pl.ds(cut * piece, piece)],
                target.at[pl.ds(cut * piece, piece)],
                sem.at[array * PIECES + cut],
            )
            copy.start()
            copies.append(copy)
    for copy in copies:
        copy.wait()


def write_out(arrays):
    return pl.pallas_call(
        write_kernel,
        out_shape=[jax.ShapeDtypeStruct(array.shape, array.dtype) for array in arrays],
        in_specs=[pl.BlockSpec(memory_space=pltpu.VMEM)] * len(arrays),
        out_specs=[pl.BlockSpec(memory_space=pltpu.HBM)] * len(arrays),
        scratch_shapes=[pltpu.SemaphoreType.DMA((len(arrays) * PIECES,))],
        compiler_params=pltpu.CompilerParams(vmem_limit_bytes=1024 * 1024),
    )(*arrays)


def on_device(
    n,
    width,
    train_query,
    low_query,
    high_query,
    train_key,
    low_key,
    high_key,
    train_value,
    low_value,
    high_value,
    train_mixed,
    low_mixed,
    high_mixed,
    norm_train,
    norm_step,
):
    norm = (norm_train + norm_step).reshape(1, -1)
    *gathered, table = gather(
        n,
        width,
        (train_mixed.T, train_query, train_key, train_value),
        (high_mixed, low_query.T, low_key.T, low_value.T),
        (low_mixed.T, high_query, high_key, high_value),
        norm,
    )
    mixed, query, key, value = write_out(gathered)
    serve_norm = table.reshape(-1).astype(jnp.bfloat16)
    return (query, key, value, mixed, serve_norm)


def solution(mesh):
    return jax.shard_map(
        functools.partial(on_device, mesh.shape["zero"], mesh.shape["width"]),
        mesh=mesh,
        in_specs=(
            P("zero", "width"),
            P("zero", None),
            P(None, "width"),
            P("zero", "width"),
            P("zero", None),
            P(None, "width"),
            P("zero", "width"),
            P("zero", None),
            P(None, "width"),
            P("width", "zero"),
            P("width", None),
            P(None, "zero"),
            P(("zero", "width")),
            P(("zero", "width")),
        ),
        out_specs=(P(None, "width"), P(None, "width"), P(None, "width"), P("width", None), P()),
        check_vma=False,
    )
```
